256 devices in a mesh: row: 8 (over y, core), col: 32 (over z, x).
Axes of the slice: x: 4, y: 4, z: 8, core: 2. Of those that a mesh axis runs over, the one named last changes fastest.
Arguments:
- rhs: bfloat16 [6144, 6144], P('row', 'col'), may hold values from -6 to 6
- basis_left: bfloat16 [6144, 6144], P('col', 'row'), may hold values from -1 to 1, as said below
- basis_right: bfloat16 [6144, 6144], P('row', 'col'), may hold values from -1 to 1, as said below
- eig_left: float32 [6144], P('row'), may hold values from 0.1 to 4
- eig_right: float32 [6144], P('col'), may hold values from 0.1 to 4
Outputs:
- solution: bfloat16 [6144, 6144], P('col', 'row')
The draws below stay inside these ranges and needn't reach their ends.
Inputs may be any that keep to these rules, and one draw needn't show every extreme that they name: `basis_left`: an orthogonal matrix drawn uniformly, rounded to bfloat16. `basis_right`: an orthogonal matrix drawn uniformly, rounded to bfloat16.
All inputs are finite; a program needn't handle non-finite values.
Results may differ from the reference program's by a relative error of at most 0.0085.
Values may be sent and summed in bfloat16 or wider, within the bound.
No kernel may reach another device: no remote copies, remote signals or barrier semaphores. Data moves between devices by JAX's collectives and lax.ppermute only.
A program may use at most 64 MiB of HBM per device.

```python
import math
import jax
import jax.numpy as jnp

N = 6144


def orthogonal_matrix(key):
    normal_draw = jax.random.normal(key, (N, N), jnp.float32)
    factor_q, factor_r = jnp.linalg.qr(normal_draw)
    signs = jnp.where(jnp.diagonal(factor_r) < 0.0, -1.0, 1.0).astype(jnp.float32)
    return (factor_q * signs[None, :]).astype(jnp.bfloat16)


def draw_basis_left(key, part):
    return orthogonal_matrix(jax.random.fold_in(key, 11))


def draw_basis_right(key, part):
    return orthogonal_matrix(jax.random.fold_in(key, 23))


def block_levels(key, shape, pieces, smallest, top_value):
    level = 1.0
    for dim, parts in pieces:
        steps = jax.random.uniform(jax.random.fold_in(jax.random.fold_in(key, 6), dim), (parts,), jnp.float32, smallest / len(pieces), top_value / len(pieces))
        level = level * jnp.repeat(jnp.exp(steps), shape[dim] // parts).reshape((-1,) + (1,) * (len(shape) - 1 - dim))
    return level


def normal_values(own_key, extent, width, reach, cuts=(), kind=jnp.bfloat16):
    loudness = block_levels(own_key, extent, cuts, -0.22, 0.18) if cuts else 1.0
    array = jax.random.normal(own_key, extent, jnp.float32) * width * loudness
    return jnp.minimum(jnp.maximum(array, -reach), reach).astype(kind)


def setup_inputs(seed: int = 0) -> dict:
    key_list = jax.random.split(jax.random.key(seed), 6)
    return {
        "rhs": normal_values(key_list[0], (N, N), 1.0, 6.0, ((0, 8), (1, 32))),
        "basis_left": draw_basis_left(jax.random.fold_in(key_list[5], 71), 0),
        "basis_right": draw_basis_right(jax.random.fold_in(key_list[5], 71), 0),
        "eig_left": jnp.clip(jnp.exp(math.log(4.0) - 3.6888794 * jax.random.uniform(key_list[3], (N,), jnp.float32) ** block_levels(key_list[3], (N,), ((0, 8),), -0.2, 0.2)), 0.1, 4.0),
        "eig_right": jnp.clip(jnp.exp(math.log(4.0) - 3.6888794 * jax.random.uniform(key_list[4], (N,), jnp.float32) ** block_levels(key_list[4], (N,), ((0, 32),), -0.2, 0.2)), 0.1, 4.0),
    }


def reference(rhs, basis_left, basis_right, eig_left, eig_right):
    projected = jnp.dot(basis_left.T.astype(jnp.float32), rhs.astype(jnp.float32), preferred_element_type=jnp.float32).astype(jnp.bfloat16)
    second = jnp.dot(projected.astype(jnp.float32), basis_right.astype(jnp.float32), preferred_element_type=jnp.float32)
    scaled = (second / (eig_left[:, None] + eig_right[None, :])).astype(jnp.bfloat16)
    half = jnp.dot(basis_left.astype(jnp.float32), scaled.astype(jnp.float32), preferred_element_type=jnp.float32).astype(jnp.bfloat16)
    return jnp.dot(half.astype(jnp.float32), basis_right.T.astype(jnp.float32), preferred_element_type=jnp.float32).astype(jnp.bfloat16)
```

```python
import jax
import jax.numpy as jnp
from jax import lax
from jax.sharding import Mesh, PartitionSpec as P

F32, BF16 = jnp.float32, jnp.bfloat16
ROW = ("y", "core")


def dot(a, b, over):
    return lax.dot_general(a, b, ((over[:1], over[1:]), ((), ())), preferred_element_type=F32)


def gathered(shard, axis, dim):
    copies = jnp.broadcast_to(shard, (lax.axis_size(axis), *shard.shape))
    parts = lax.all_to_all(copies, axis, 0, 0, tiled=True)
    if dim == 0:
        return parts.reshape(-1, parts.shape[-1])
    return jnp.moveaxis(parts, 0, 1).reshape(parts.shape[1], -1)


def summed(partial, axis):
    peers = lax.axis_size(axis)
    parts = partial.reshape(peers, partial.shape[0] // peers, partial.shape[1])
    parts = lax.all_to_all(parts, axis, 0, 0, tiled=True)
    return jnp.sum(parts.astype(F32), axis=0)


def body(rhs, basis_left, basis_right, eig_left, eig_right):
    row_of = [(z * 8 + r, r * 8 + z) for z in range(8) for r in range(8)]
    left = lax.all_gather(basis_left, "z", axis=0, tiled=True)
    c_part = lax.all_to_all(rhs, "x", 0, 1, tiled=True)
    c_block = gathered(c_part, ROW, 0)
    turned = lax.ppermute(basis_right, (*ROW, "z"), row_of)
    right = lax.all_gather(turned, ROW, axis=1, tiled=True)
    part = dot(left, c_block, (0, 0)).astype(BF16)
    projected = gathered(summed(part, "x").astype(BF16), "x", 0)
    part = dot(projected, right, (1, 0)).astype(BF16)
    second = lax.psum_scatter(part, "z", scatter_dimension=1, tiled=True).astype(F32)
    scaled = (second / (eig_left[:, None] + eig_right[None, :])).astype(BF16)
    basis_right, _ = lax.optimization_barrier((basis_right, part))
    right = lax.all_gather(basis_right, "x", axis=1, tiled=True)
    scaled = gathered(scaled, "x", 1)
    part = dot(left, scaled, (1, 0)).astype(BF16)
    half = summed(part, "core").astype(BF16)
    half = summed(half, "y").astype(BF16)
    half = gathered(gathered(half, "y", 0), "core", 0)
    part = dot(half, right, (1, 1)).astype(BF16)
    return lax.psum_scatter(part, "z", scatter_dimension=0, tiled=True)


def solution(mesh):
    split = Mesh(mesh.devices.reshape(4, 2, 8, 4), ("y", "core", "z", "x"))
    row, col = ROW, ("z", "x")
    in_specs = (P(row, col), P(col, row), P(row, col), P(row), P(col))
    return jax.shard_map(body, mesh=split, in_specs=in_specs, out_specs=P(col, row), check_vma=False)
```

```python
import jax
import jax.numpy as jnp
from jax import lax
from jax.experimental.layout import Layout, with_layout_constraint
from jax.sharding import Mesh, PartitionSpec as P

F32, BF16 = jnp.float32, jnp.bfloat16
ROW = ("y", "core")


def dot(a, b, over):
    return lax.dot_general(a, b, ((over[:1], over[1:]), ((), ())), preferred_element_type=F32)


def gathered_parts(shard, axis):
    copies = jnp.broadcast_to(shard, (lax.axis_size(axis), *shard.shape))
    return lax.all_to_all(copies, axis, 0, 0, tiled=True)


def gathered(shard, axis, dim):
    parts = gathered_parts(shard, axis)
    if dim == 0:
        return parts.reshape(-1, parts.shape[-1])
    return jnp.moveaxis(parts, 0, 1).reshape(parts.shape[1], -1)


def summed(partial, axis):
    peers = lax.axis_size(axis)
    parts = partial.reshape(peers, partial.shape[0] // peers, partial.shape[1])
    parts = lax.all_to_all(parts, axis, 0, 0, tiled=True)
    return jnp.sum(parts.astype(F32), axis=0)


def shifted(value, axis, by):
    peers = lax.axis_size(axis)
    return lax.ppermute(value, axis, [(i, (i + by) % peers) for i in range(peers)])


def ring_blocks(own, axis):
    far = lax.axis_size(axis) // 2
    blocks = {0: own}
    up = down = own
    for k in range(1, far):
        up, down = shifted(up, axis, 1), shifted(down, axis, -1)
        blocks[-k], blocks[k] = up, down
    half = own.shape[0] // 2
    up, down = shifted(up[:half], axis, 1), shifted(down[half:], axis, -1)
    blocks[far] = jnp.concatenate([up, down])
    return blocks


def ring_sum(term, axis, cut):
    far = lax.axis_size(axis) // 2
    terms = {k: lax.optimization_barrier(term(k)) for k in range(1 - far, far + 1)}

    def halves(value):
        return jnp.split(value, 2, axis=cut)

    low, high = halves(terms[far])
    up = shifted(low.astype(BF16), axis, 1)
    down = shifted(high.astype(BF16), axis, -1)
    low, high = halves(terms[far - 1])
    up = jnp.concatenate([(low + up).astype(BF16), high.astype(BF16)], axis=cut)
    low, high = halves(terms[1 - far])
    down = jnp.concatenate([low.astype(BF16), (high + down).astype(BF16)], axis=cut)
    for k in range(far - 2, -1, -1):
        up, down = shifted(up, axis, 1), shifted(down, axis, -1)
        if k:
            up, down = (terms[k] + up).astype(BF16), (terms[-k] + down).astype(BF16)
    return terms[0] + up + down


def body(rhs, basis_left, basis_right, eig_left, eig_right):
    z, y, core = (lax.axis_index(axis) for axis in ("z", "y", "core"))

    def block(value, at):
        return lax.dynamic_slice_in_dim(value, at * 192, 192, 0)

    left = lax.all_gather(basis_left, "z", axis=0, tiled=True)
    both = jnp.concatenate([rhs.T, basis_right.T]).reshape(2, 192, 4, 192)
    both = lax.all_to_all(both, "x", 2, 2, tiled=True)
    c_block, right_x = both.transpose(0, 3, 2, 1).reshape(2, 192, 768)
    c_block = gathered_parts(gathered_parts(c_block, "y"), "core")
    c_block = c_block.reshape(2, 4, 192, 768).swapaxes(0, 1).reshape(1536, 768)
    right_x = lax.all_gather(right_x, ROW, axis=0, tiled=True)
    part = dot(c_block, left, (0, 0))
    projected = summed(part.astype(BF16), "x").astype(BF16)
    part = 0.0
    for k, term in ring_blocks(projected, "z").items():
        part += dot(block(right_x, (z + k + 8) % 8), term, (0, 0))
    second = summed(part.astype(BF16), "x")
    scaled = (second / (eig_right[:, None] + eig_left[None, :])).astype(BF16)
    right, _ = lax.optimization_barrier((basis_right, projected))
    right = lax.all_gather(right, "x", axis=1, tiled=True)
    scaled = gathered(scaled, "x", 0)
    part = dot(left, scaled, (1, 1)).astype(BF16)
    part = with_layout_constraint(part, Layout((0, 1)))
    part = lax.all_to_all(part.reshape(2, 768, 768), "core", 0, 0, tiled=True)

    def half_term(k):
        at = (y + k + 4) % 4
        return block(part[0], at).astype(F32) + block(part[1], at)

    half = ring_blocks(ring_sum(half_term, "y", 1).astype(BF16), "y")
    half = jnp.concatenate([half[k] for k in (0, 1, 2, -1)])
    half = jnp.concatenate([half, shifted(half, "core", 1)])

    def term(k):
        at = (z + k + 8) % 8
        return dot(block(half, (at // 4 + core) % 2 * 4 + (at + 4 - y) % 4), right, (1, 1))

    return ring_sum(term, "z", 1).astype(BF16)


def solution(mesh):
    split = Mesh(mesh.devices.reshape(4, 2, 8, 4), ("y", "core", "z", "x"))
    row, col = ROW, ("z", "x")
    in_specs = (P(row, col), P(col, row), P(row, col), P(row), P(col))
    return jax.shard_map(body, mesh=split, in_specs=in_specs, out_specs=P(col, row), check_vma=False)
```

```python
import jax
import jax.numpy as jnp
from jax import lax
from jax.experimental.layout import Layout, with_layout_constraint
from jax.sharding import Mesh, PartitionSpec as P

F32, BF16 = jnp.float32, jnp.bfloat16
ROW = ("y", "core")


def dot(a, b, over):
    return lax.dot_general(a, b, ((over[:1], over[1:]), ((), ())), preferred_element_type=F32)


def gathered_parts(shard, axis):
    copies = jnp.broadcast_to(shard, (lax.axis_size(axis), *shard.shape))
    return lax.all_to_all(copies, axis, 0, 0, tiled=True)


def gathered(shard, axis, dim):
    parts = gathered_parts(shard, axis)
    if dim == 0:
        return parts.reshape(-1, parts.shape[-1])
    return jnp.moveaxis(parts, 0, 1).reshape(parts.shape[1], -1)


def summed(partial, axis):
    peers = lax.axis_size(axis)
    parts = partial.reshape(peers, partial.shape[0] // peers, partial.shape[1])
    parts = lax.all_to_all(parts, axis, 0, 0, tiled=True)
    return jnp.sum(parts.astype(F32), axis=0)


def shifted(value, axis, by):
    peers = lax.axis_size(axis)
    return lax.ppermute(value, axis, [(i, (i + by) % peers) for i in range(peers)])


def ring_blocks(own, axis):
    far = lax.axis_size(axis) // 2
    blocks = {0: own}
    up = down = own
    for k in range(1, far):
        up, down = shifted(up, axis, 1), shifted(down, axis, -1)
        blocks[-k], blocks[k] = up, down
    half = own.shape[0] // 2
    up, down = shifted(up[:half], axis, 1), shifted(down[half:], axis, -1)
    blocks[far] = jnp.concatenate([up, down])
    return blocks


def ring_sum(term, axis, cut):
    far = lax.axis_size(axis) // 2
    terms = {k: lax.optimization_barrier(term(k)) for k in range(1 - far, far + 1)}

    def halves(value):
        return jnp.split(value, 2, axis=cut)

    low, high = halves(terms[far])
    up = shifted(low.astype(BF16), axis, 1)
    down = shifted(high.astype(BF16), axis, -1)
    low, high = halves(terms[far - 1])
    up = jnp.concatenate([(low + up).astype(BF16), high.astype(BF16)], axis=cut)
    low, high = halves(terms[1 - far])
    down = jnp.concatenate([low.astype(BF16), (high + down).astype(BF16)], axis=cut)
    for k in range(far - 2, -1, -1):
        up, down = shifted(up, axis, 1), shifted(down, axis, -1)
        if k:
            up, down = (terms[k] + up).astype(BF16), (terms[-k] + down).astype(BF16)
    return terms[0] + up + down


def placed(buffer, rows, at):
    return lax.dynamic_update_slice_in_dim(buffer, rows, at, 0)


def body(rhs, basis_left, basis_right, eig_left, eig_right):
    z, y, core = (lax.axis_index(axis) for axis in ("z", "y", "core"))

    def block(value, at):
        return lax.dynamic_slice_in_dim(value, at * 192, 192, 0)

    left = lax.all_gather(basis_left, "z", axis=0, tiled=True)
    both = jnp.concatenate([rhs.T, basis_right.T]).reshape(2, 192, 4, 192)
    both = lax.all_to_all(both, "x", 2, 2, tiled=True)
    c_block, right_x = both.transpose(0, 3, 2, 1).reshape(2, 192, 768)
    c_block = gathered_parts(gathered_parts(c_block, "y"), "core")
    c_block = c_block.reshape(2, 4, 192, 768).swapaxes(0, 1).reshape(1536, 768)
    right_x = lax.all_gather(right_x, ROW, axis=0, tiled=True)
    part = dot(c_block, left, (0, 0))
    projected = summed(part.astype(BF16), "x").astype(BF16)
    part = 0.0
    for k, term in ring_blocks(projected, "z").items():
        part += dot(block(right_x, (z + k + 8) % 8), term, (0, 0))
    second = summed(part.astype(BF16), "x")
    scaled = (second / (eig_right[:, None] + eig_left[None, :])).astype(BF16)
    right, _ = lax.optimization_barrier((basis_right, projected))
    right = lax.all_gather(right, "x", axis=1, tiled=True)
    scaled = gathered(scaled, "x", 0)
    part = dot(left, scaled, (1, 1)).astype(BF16)
    part = with_layout_constraint(part, Layout((0, 1)))
    part = lax.all_to_all(part.reshape(2, 768, 768), "core", 0, 0, tiled=True)

    def half_term(k):
        at = (y + k + 4) % 4
        return block(part[0], at).astype(F32) + block(part[1], at)

    half = ring_blocks(ring_sum(half_term, "y", 1).astype(BF16), "y")
    mine = jnp.zeros((768, 768), BF16)
    for k, rows in half.items():
        mine = placed(mine, rows, (y + k + 4) % 4 * 192)
    half = placed(jnp.zeros((1536, 768), BF16), mine, core * 768)
    half = placed(half, shifted(mine, "core", 1), (1 - core) * 768)
    term = lambda k: dot(block(half, (z + k + 8) % 8), right, (1, 1))
    return ring_sum(term, "z", 1).astype(BF16)


def solution(mesh):
    split = Mesh(mesh.devices.reshape(4, 2, 8, 4), ("y", "core", "z", "x"))
    row, col = ROW, ("z", "x")
    in_specs = (P(row, col), P(col, row), P(row, col), P(row), P(col))
    return jax.shard_map(body, mesh=split, in_specs=in_specs, out_specs=P(col, row), check_vma=False)
```
